32 devices in a mesh: band: 8 (over y, x, core), gslab: 4 (over z).
Axes of the slice: x: 2, y: 2, z: 4, core: 2. Of those that a mesh axis runs over, the one named last changes fastest.
Arguments:
- band_coeffs: float32 [3072, 49152], P('band', 'gslab'), may hold values from -6 to 6
- sign_table: int32 [12, 3072], P(None, 'band'), may hold values from -1 to 1, as said below
- slice_widths: int32 [16], replicated, may hold values from 96 to 384, as said below
- owner_map: int32 [16], replicated, may hold values from 0 to 15, each once
Outputs:
- pseudobands: float32 [192, 49152], P(('band', 'gslab'))
The draws below stay inside these ranges and needn't reach their ends.
Inputs may be any that keep to these rules, and one draw needn't show every extreme that they name: `sign_table`: every entry is -1 or 1. `slice_widths`: the widths sum to 3072; every slice holds 96 to 384 bands, and in every draw some slice holds exactly 96 and some exactly 384. `owner_map`: each slice appears once.
All inputs are finite; a program needn't handle non-finite values.
Results may differ from the reference program's by a relative error of at most 0.0003.
Values sent between devices are 32-bit elements; how exact they have to be, the bound alone decides.
A program may use at most 128 MiB of HBM per device.

```python
import jax
import jax.numpy as jnp
from jax import lax

NG = 49152
BANDS_DEV = 384
SLICE_BAND = 2
NPS = 12
NB = 3072
NSLICE = 16
MOST = 384
NPB = 192


def draw_sign_table(key, part):
    return (2 * jax.random.randint(jax.random.fold_in(key, 17), (NPS, NB), 0, 2) - 1).astype(jnp.int32)


def draw_slice_widths(key, part):
    average = BANDS_DEV // SLICE_BAND
    narrow = average // 2
    place = jax.random.randint(jax.random.fold_in(key, 3), (), 0, NSLICE - 3)
    positions = jnp.arange(NSLICE, dtype=jnp.int32)
    relative = positions - place
    special = (relative >= 0) & (relative < 4)
    ranking = jnp.where(positions < place, positions, positions - 4)
    ranking = jnp.maximum(ranking, 0)
    pair_id = jnp.minimum(ranking // 2, NSLICE // 2 - 1)
    parity = ranking % 2
    spread = jax.random.randint(jax.random.fold_in(key, 5), (NSLICE // 2,), -(average - narrow), average - narrow + 1)
    shift_value = spread[pair_id]
    drawn = average + jnp.where(parity == 0, shift_value, -shift_value)
    table = jnp.array([narrow, 2 * average, narrow, average], dtype=jnp.int32)
    marked = table[jnp.clip(relative, 0, 3)]
    return jnp.where(special, marked, drawn).astype(jnp.int32)


def block_levels(key, extent, split, low, largest):
    level, own = 1.0, jax.random.fold_in(key, 6)
    for position, blocks in split:
        draws = jnp.exp(jax.random.uniform(jax.random.fold_in(own, position), (blocks,), jnp.float32, low / len(split), largest / len(split)))
        level = level * jnp.repeat(draws, extent[position] // blocks).reshape([-1 if axis == position else 1 for axis in range(len(extent))])
    return level


def centred(rng, shape, width, most, split=(), kind=jnp.bfloat16):
    values = width * jax.random.normal(rng, shape, jnp.float32)
    if split:
        values = values * block_levels(rng, shape, split, -0.22, 0.18)
    return jnp.clip(values, -most, most).astype(kind)


def setup_inputs(seed: int = 0) -> dict:
    key_of = jax.random.split(jax.random.key(seed), 5)
    return {
        "band_coeffs": centred(key_of[0], (NB, NG), 1.0, 6.0, ((0, 8), (1, 4)), jnp.float32),
        "sign_table": draw_sign_table(jax.random.fold_in(key_of[4], 71), 0),
        "slice_widths": draw_slice_widths(jax.random.fold_in(key_of[4], 71), 0),
        "owner_map": jax.random.permutation(key_of[3], NSLICE).astype(jnp.int32),
    }


def reference(band_coeffs, sign_table, slice_widths, owner_map):
    ends = jnp.cumsum(slice_widths).astype(jnp.int32)
    starts = (ends - slice_widths).astype(jnp.int32)
    inverse = 1.0 / jnp.sqrt(slice_widths.astype(jnp.float32))

    def one_slice(slice_id):
        begin = starts[slice_id]
        finish = ends[slice_id]
        window_start = jnp.minimum(begin, NB - MOST).astype(jnp.int32)
        block = lax.dynamic_slice(band_coeffs, (window_start, jnp.int32(0)), (MOST, NG))
        band_ids = window_start + jnp.arange(MOST, dtype=jnp.int32)
        inside = (band_ids >= begin) & (band_ids < finish)
        sign_block = lax.dynamic_slice(sign_table, (jnp.int32(0), window_start), (NPS, MOST)).astype(jnp.float32)
        weights = jnp.where(inside[None, :], sign_block * inverse[slice_id], jnp.zeros_like(sign_block))
        return jnp.dot(weights, block, precision=lax.Precision.HIGHEST, preferred_element_type=jnp.float32)
    result = lax.map(one_slice, jnp.arange(NSLICE, dtype=jnp.int32))
    return result[owner_map].reshape(NPB, NG)
```

```python
import functools

import jax
import jax.numpy as jnp
from jax import lax
from jax.experimental import pallas as pl
from jax.experimental.pallas import tpu as pltpu
from jax.sharding import PartitionSpec as P

NARROWEST = 96
LANES = 128
SUBLANES = 8
HALF = 4
VMEM = 67043328
MERGE_LAG = 2
FINISH_LAG = 4
UNPACK_LAG = 8
MESH = pl.DeviceIdType.MESH


def mixing_rows(row_ids, slice_of_band, sign_float, owner_map, inverse, per_slice):
    slice_count = owner_map.shape[0]
    slot_group = row_ids // per_slice
    within = row_ids % per_slice
    slice_range = jnp.arange(slice_count, dtype=jnp.int32)
    picked = slot_group[:, None] == slice_range[None, :]
    target = jnp.sum(jnp.where(picked, owner_map[None, :], 0), axis=1)
    member = target[:, None] == slice_range[None, :]
    row_scale = jnp.sum(jnp.where(member, inverse[None, :], 0.0), axis=1)
    one_hot = (within[:, None] == jnp.arange(per_slice, dtype=jnp.int32)[None, :]).astype(
        jnp.float32
    )
    sign_rows = jnp.dot(
        one_hot, sign_float, precision=lax.Precision.HIGHEST, preferred_element_type=jnp.float32
    )
    return jnp.where(slice_of_band[None, :] == target[:, None], sign_rows * row_scale[:, None], 0.0)


def dense(band_coeffs, sign_table, slice_widths, owner_map):
    local_bands = band_coeffs.shape[0]
    per_slice = sign_table.shape[0]
    slice_count = owner_map.shape[0]
    total_rows = slice_count * per_slice
    first_band = lax.axis_index("band") * local_bands
    band_ids = first_band + jnp.arange(local_bands, dtype=jnp.int32)
    ends = jnp.cumsum(slice_widths)
    slice_of_band = jnp.sum((band_ids[:, None] >= ends[None, :]).astype(jnp.int32), axis=1)
    inverse = 1.0 / jnp.sqrt(slice_widths.astype(jnp.float32))
    sign_float = sign_table.astype(jnp.float32)
    row_ids = jnp.arange(total_rows, dtype=jnp.int32)
    mixing = mixing_rows(row_ids, slice_of_band, sign_float, owner_map, inverse, per_slice)
    summed = lax.psum_scatter(
        jnp.dot(
            mixing, band_coeffs, precision=lax.Precision.HIGHEST, preferred_element_type=jnp.float32
        ),
        "band",
        scatter_dimension=0,
        tiled=True,
    )
    return lax.all_to_all(summed, "gslab", split_axis=0, concat_axis=1, tiled=True)


def two_term_dot(exact, values):
    high = values.astype(jnp.bfloat16)
    low = (values - high.astype(jnp.float32)).astype(jnp.bfloat16)
    return jnp.dot(exact, high, preferred_element_type=jnp.float32) + jnp.dot(
        exact, low, preferred_element_type=jnp.float32
    )


def kernel(
    slabs, chunks, reach,
    widths_ref, owner_ref, signs_ref, band_ref, out_ref,
    held, mix, sent, got, chosen, scale, half, came, done, parcel,
    load_sem, send1, recv1, send2, recv2, send3, recv3, near,
):
    my_group = lax.axis_index("band")
    my_slab = lax.axis_index("gslab")
    my_core = lax.rem(my_group, 2)
    bits = (my_group // 4, lax.rem(my_group // 2, 2))
    per_slice, local_bands = signs_ref.shape
    slices = widths_ref.shape[0]
    packed, width = sent.shape[2:]
    peers = done.shape[1]
    mine = out_ref.shape[0]
    extra = mine - HALF
    tall_block = mine * slabs
    tiles = slabs - 1
    live = reach * per_slice

    def group_of(axis, along, other, core):
        return along * 4 + other * 2 + core if axis == 0 else other * 4 + along * 2 + core

    def own(axis):
        return bits[axis], bits[1 - axis]

    def here_at(axis):
        return own(axis)[0] * 2 + my_core

    def quarter_at(axis, k):
        return lax.rem(own(axis)[0] * 2 + 2 + k // 2 * 2, 4) + lax.rem(my_core + k + k // 2, 2)

    def load(chunk, quarter):
        start = (quarter * chunks + chunk) * width
        return pltpu.make_async_copy(
            band_ref.at[:, pl.ds(pl.multiple_of(start, width), width)],
            held.at[chunk, quarter],
            load_sem.at[chunk % 3],
        )

    def load_chunk(chunk):
        for quarter in range(4):
            load(chunk, quarter).start()

    def wait_load(chunk):
        pltpu.make_async_copy(held.at[chunk], held.at[chunk], load_sem.at[chunk % 3]).wait()

    load_chunk(0)

    barrier = pltpu.get_barrier_semaphore()

    def greet(semaphore, group, slab):
        pl.semaphore_signal(
            semaphore, inc=1, device_id={"band": group, "gslab": slab}, device_id_type=MESH
        )

    inner = lax.rem(my_slab + slabs - 1, slabs) // tiles
    outer = my_slab // tiles
    sides = 2 - inner - outer

    def greet_sides(semaphore):
        @pl.when(my_slab > 0)
        def _():
            greet(semaphore, my_group, my_slab - 1)

        @pl.when(my_slab < slabs - 1)
        def _():
            greet(semaphore, my_group, my_slab + 1)

    greet(barrier, group_of(0, bits[0], bits[1], 1 - my_core), my_slab)
    for axis in range(2):
        along, other = own(axis)
        for core in range(2):
            greet(barrier, group_of(axis, 1 - along, other, core), my_slab)
    greet_sides(barrier)
    load_chunk(1)

    ends = []
    running = jnp.int32(0)
    for s in range(slices):
        running = running + widths_ref[s]
        ends.append(running)

    first_band = my_group * local_bands
    bands = first_band + lax.broadcasted_iota(jnp.int32, (1, local_bands), 1)
    slice_of = jnp.zeros((1, local_bands), jnp.int32)
    first = jnp.int32(0)
    for s in range(slices):
        slice_of = slice_of + jnp.where(bands >= ends[s], 1, 0)
        first = first + jnp.where(first_band >= ends[s], 1, 0)
    row = lax.broadcasted_iota(jnp.int32, (packed, per_slice), 0)
    column = lax.broadcasted_iota(jnp.int32, (packed, per_slice), 1)
    repeat = jnp.where(lax.rem(row, per_slice) == column, 1.0, 0.0).astype(jnp.float32)
    signs = jnp.dot(
        repeat, signs_ref[...].astype(jnp.float32), preferred_element_type=jnp.float32
    )
    row = lax.broadcasted_iota(jnp.int32, (packed, local_bands), 0)
    hit = (slice_of - first == row // per_slice) & (row < live)
    mix[...] = jnp.where(hit, signs, 0.0).astype(jnp.bfloat16)

    def exchange(chunk, quarter, source):
        axis = chunk % 2
        return pltpu.make_async_remote_copy(
            src_ref=sent.at[chunk, quarter],
            dst_ref=got.at[chunk, source],
            send_sem=send1,
            recv_sem=recv1.at[chunk],
            device_id={
                "band": group_of(axis, quarter // 2, own(axis)[1], lax.rem(quarter, 2)),
                "gslab": my_slab,
            },
            device_id_type=MESH,
        )

    def send_partial(chunk):
        if chunk + 2 < chunks:
            load_chunk(chunk + 2)
        wait_load(chunk)
        axis = chunk % 2
        here = here_at(axis)

        @pl.loop(0, 3)
        def _(k):
            quarter = quarter_at(axis, k)
            sent[chunk, quarter] = two_term_dot(mix[...], held[chunk, quarter])
            if chunk:
                exchange(chunk, quarter, here).start()

        got[chunk, here] = two_term_dot(mix[...], held[chunk, here])

    def cross(chunk):
        axis = chunk % 2
        along, other = own(axis)
        return pltpu.make_async_remote_copy(
            src_ref=half.at[chunk, 0],
            dst_ref=came.at[chunk],
            send_sem=send2,
            recv_sem=recv2.at[chunk],
            device_id={"band": group_of(axis, along, 1 - other, my_core), "gslab": my_slab},
            device_id_type=MESH,
        )

    def wait_bytes(ref, semaphore):
        pltpu.make_async_copy(ref, ref, semaphore).wait()

    def merge(chunk):
        wait_bytes(got.at[chunk, pl.ds(0, 3)], recv1.at[chunk])
        rows = got[chunk].reshape(4 * packed, width)
        value = two_term_dot(chosen[chunk % 2], rows)
        half[chunk] = value.reshape(2, peers * mine, width)
        cross(chunk).start()

    def deliver(chunk, slab, quarter):
        axis = chunk % 2
        return pltpu.make_async_remote_copy(
            src_ref=done.at[chunk, quarter * slabs + slab],
            dst_ref=parcel.at[my_slab, here_at(axis), chunk],
            send_sem=send3,
            recv_sem=recv3.at[chunk],
            device_id={
                "band": group_of(axis, quarter // 2, own(axis)[1], lax.rem(quarter, 2)),
                "gslab": slab,
            },
            device_id_type=MESH,
        )

    def finish(chunk):
        axis = chunk % 2
        here = here_at(axis)
        cross(chunk).wait_recv()
        total = (half[chunk, 1] + came[chunk]) * scale[axis, :, :1]
        total = total.reshape(4 * tiles, SUBLANES, width)
        level = lax.broadcasted_iota(jnp.int32, (SUBLANES, LANES), 0)
        early = level % HALF < extra
        for quarter in range(4):
            tile = [total[quarter * tiles + k] for k in range(tiles)]
            left = [t[:, :LANES] for t in tile]
            right = [t[:, LANES:] for t in tile]
            even = jnp.where(early, left[-1], pltpu.roll(right[-1], extra, 0))
            odd = jnp.where(early, pltpu.roll(left[-1], SUBLANES - extra, 0), right[-1])
            for slab in range(slabs):
                at = slab % 2 * HALF
                end = slab // 2 * HALF
                peer = quarter * slabs + slab
                done[chunk, peer, 0] = left[slab // 2][at:at + HALF]
                done[chunk, peer, 1] = right[slab // 2][at:at + HALF]
                done[chunk, peer, 2] = (odd if slab % 2 else even)[end:end + HALF]
        pltpu.make_async_copy(
            done.at[chunk, here * slabs + my_slab], parcel.at[my_slab, here, chunk], recv3.at[chunk]
        ).start()
        side = my_slab // 2

        @pl.loop(0, 8)
        def _(k):
            deliver(chunk, 2 - 2 * side + k // 4, lax.rem(here + k, 4)).start()

        @pl.loop(0, 4)
        def _(k):
            deliver(chunk, 4 * side + 1 - my_slab, lax.rem(here + k, 4)).start()

        @pl.loop(1, 4)
        def _(k):
            deliver(chunk, my_slab, lax.rem(here + k, 4)).start()

    def unpack(chunk):
        wait_bytes(parcel.at[:, :, chunk], recv3.at[chunk])
        for slab in range(slabs):
            for quarter in range(4):
                at = ((slab * 4 + quarter) * chunks + chunk) * width
                left, right = slice(at, at + LANES), slice(at + LANES, at + 2 * LANES)
                out_ref[:HALF, left] = parcel[slab, quarter, chunk, 0]
                out_ref[:HALF, right] = parcel[slab, quarter, chunk, 1]
                out_ref[HALF:, left] = parcel[slab, quarter, chunk, 2, :extra]
                out_ref[HALF:, right] = parcel[slab, quarter, chunk, 2, extra:]

    send_partial(0)
    pl.semaphore_wait(barrier, 5 + sides)

    @pl.loop(0, 3)
    def _(k):
        exchange(0, quarter_at(0, k), here_at(0)).start()

    greet_sides(near.at[0])

    for axis in range(2):
        along, other = own(axis)
        shape = (2 * peers * mine, 1)
        tall = lax.broadcasted_iota(jnp.int32, shape, 0)
        stays = tall // (peers * mine)
        rest = lax.rem(tall, peers * mine)
        quarter = rest // tall_block
        rest = lax.rem(rest, tall_block)
        low = rest < slabs * HALF
        beyond = rest - slabs * HALF
        slab = jnp.where(low, rest // HALF, beyond // extra)
        within = jnp.where(low, lax.rem(rest, HALF), HALF + lax.rem(beyond, extra))
        side = jnp.where(stays == 1, other, 1 - other)
        group = group_of(axis, quarter // 2, side, lax.rem(quarter, 2))
        output_row = (group * slabs + slab) * mine + within
        block = output_row // per_slice
        target = jnp.zeros(shape, jnp.int32)
        for s in range(slices):
            target = jnp.where(block == s, owner_ref[s], target)
        breadth = jnp.ones(shape, jnp.int32)
        for s in range(slices):
            breadth = jnp.where(target == s, widths_ref[s], breadth)
        root = 1.0 / jnp.sqrt(breadth.astype(jnp.float32))
        scale[axis] = jnp.broadcast_to(root[peers * mine:], (peers * mine, LANES))
        wanted = target * per_slice + lax.rem(output_row, per_slice)
        wide = lax.broadcasted_iota(jnp.int32, (1, 4 * packed), 1)
        place = lax.rem(wide, packed)
        quarter = wide // packed
        begin = group_of(axis, quarter // 2, other, lax.rem(quarter, 2)) * local_bands
        lowest = jnp.zeros((1, 4 * packed), jnp.int32)
        for s in range(slices):
            lowest = lowest + jnp.where(begin >= ends[s], 1, 0)
        offered = jnp.where(place < live, lowest * per_slice + place, -2)
        chosen[axis] = jnp.where(wanted == offered, 1.0, 0.0).astype(jnp.bfloat16)

    known = 0

    def learn():
        pl.semaphore_wait(near.at[known], sides)
        if known + 1 < tiles:
            greet_sides(near.at[known + 1])

    for step in range(1, chunks + UNPACK_LAG):
        if step < chunks:
            send_partial(step)
        if known < tiles:
            learn()
            known += 1
        if 0 <= step - MERGE_LAG < chunks:
            merge(step - MERGE_LAG)
        if 0 <= step - FINISH_LAG < chunks:
            finish(step - FINISH_LAG)
        if 0 <= step - UNPACK_LAG < chunks:
            unpack(step - UNPACK_LAG)

    wait_bytes(sent.at[:, pl.ds(0, 3)], send1)
    wait_bytes(came, send2)
    wait_bytes(done.at[:, pl.ds(0, peers - 1)], send3)


def on_device(groups, slabs, band_coeffs, sign_table, slice_widths, owner_map):
    local_bands, local_columns = band_coeffs.shape
    per_slice = sign_table.shape[0]
    rows = owner_map.shape[0] * per_slice
    width = 2 * LANES
    chunks, odd = divmod(local_columns, 4 * width)
    mine = rows // (8 * slabs)
    fits = 2 * (mine - HALF) == HALF and slabs == HALF
    if groups != 8 or odd or rows % (8 * slabs) or not fits:
        return dense(band_coeffs, sign_table, slice_widths, owner_map)
    reach = (local_bands - 2) // NARROWEST + 2
    packed = -(-reach * per_slice // 8) * 8
    peers = 4 * slabs
    return pl.pallas_call(
        functools.partial(kernel, slabs, chunks, reach),
        out_shape=pltpu.VMEM((mine, local_columns * slabs), jnp.float32),
        in_specs=[
            pl.BlockSpec(memory_space=pltpu.SMEM),
            pl.BlockSpec(memory_space=pltpu.SMEM),
            pl.BlockSpec(memory_space=pltpu.VMEM),
            pl.BlockSpec(memory_space=pl.ANY),
        ],
        out_specs=pl.BlockSpec(memory_space=pltpu.VMEM),
        scratch_shapes=[
            pltpu.VMEM((chunks, 4, local_bands, width), jnp.float32),
            pltpu.VMEM((packed, local_bands), jnp.bfloat16),
            pltpu.VMEM((chunks, 4, packed, width), jnp.float32),
            pltpu.VMEM((chunks, 4, packed, width), jnp.float32),
            pltpu.VMEM((2, 2 * peers * mine, 4 * packed), jnp.bfloat16),
            pltpu.VMEM((2, peers * mine, LANES), jnp.float32),
            pltpu.VMEM((chunks, 2, peers * mine, width), jnp.float32),
            pltpu.VMEM((chunks, peers * mine, width), jnp.float32),
            pltpu.VMEM((chunks, peers, 3, HALF, LANES), jnp.float32),
            pltpu.VMEM((slabs, 4, chunks, 3, HALF, LANES), jnp.float32),
            pltpu.SemaphoreType.DMA((3,)),
            pltpu.SemaphoreType.DMA,
            pltpu.SemaphoreType.DMA((chunks,)),
            pltpu.SemaphoreType.DMA,
            pltpu.SemaphoreType.DMA((chunks,)),
            pltpu.SemaphoreType.DMA,
            pltpu.SemaphoreType.DMA((chunks,)),
            pltpu.SemaphoreType.REGULAR((slabs - 1,)),
        ],
        compiler_params=pltpu.CompilerParams(
            collective_id=0, has_side_effects=True, vmem_limit_bytes=VMEM - 8 * local_columns * slabs * 4
        ),
        name="pseudobands",
    )(slice_widths, owner_map, sign_table, band_coeffs)


def solution(mesh):
    return jax.shard_map(
        functools.partial(on_device, mesh.shape["band"], mesh.shape["gslab"]),
        mesh=mesh,
        in_specs=(P("band", "gslab"), P(None, "band"), P(), P()),
        out_specs=P(("band", "gslab"), None),
        check_vma=False,
    )
```

```python
import functools

import jax
import jax.numpy as jnp
from jax import lax
from jax.experimental import pallas as pl
from jax.experimental.pallas import tpu as pltpu
from jax.sharding import PartitionSpec as P

NARROWEST = 96
LANES = 128
SUBLANES = 8
HALF = 4
VMEM = 67043328
CHUNK_REFS = ("held", "sent", "got", "half", "came", "done", "parcel")
NARROW = 2
MERGE_LAG = 2
FINISH_LAG = 4
UNPACK_LAG = 7
MESH = pl.DeviceIdType.MESH


def mixing_rows(row_ids, slice_of_band, sign_float, owner_map, inverse, per_slice):
    slice_count = owner_map.shape[0]
    slot_group = row_ids // per_slice
    within = row_ids % per_slice
    slice_range = jnp.arange(slice_count, dtype=jnp.int32)
    picked = slot_group[:, None] == slice_range[None, :]
    target = jnp.sum(jnp.where(picked, owner_map[None, :], 0), axis=1)
    member = target[:, None] == slice_range[None, :]
    row_scale = jnp.sum(jnp.where(member, inverse[None, :], 0.0), axis=1)
    one_hot = (within[:, None] == jnp.arange(per_slice, dtype=jnp.int32)[None, :]).astype(
        jnp.float32
    )
    sign_rows = jnp.dot(
        one_hot, sign_float, precision=lax.Precision.HIGHEST, preferred_element_type=jnp.float32
    )
    return jnp.where(slice_of_band[None, :] == target[:, None], sign_rows * row_scale[:, None], 0.0)


def dense(band_coeffs, sign_table, slice_widths, owner_map):
    local_bands = band_coeffs.shape[0]
    per_slice = sign_table.shape[0]
    slice_count = owner_map.shape[0]
    total_rows = slice_count * per_slice
    first_band = lax.axis_index("band") * local_bands
    band_ids = first_band + jnp.arange(local_bands, dtype=jnp.int32)
    ends = jnp.cumsum(slice_widths)
    slice_of_band = jnp.sum((band_ids[:, None] >= ends[None, :]).astype(jnp.int32), axis=1)
    inverse = 1.0 / jnp.sqrt(slice_widths.astype(jnp.float32))
    sign_float = sign_table.astype(jnp.float32)
    row_ids = jnp.arange(total_rows, dtype=jnp.int32)
    mixing = mixing_rows(row_ids, slice_of_band, sign_float, owner_map, inverse, per_slice)
    summed = lax.psum_scatter(
        jnp.dot(
            mixing, band_coeffs, precision=lax.Precision.HIGHEST, preferred_element_type=jnp.float32
        ),
        "band",
        scatter_dimension=0,
        tiled=True,
    )
    return lax.all_to_all(summed, "gslab", split_axis=0, concat_axis=1, tiled=True)


def two_term_dot(exact, values):
    high = values.astype(jnp.bfloat16)
    low = (values - high.astype(jnp.float32)).astype(jnp.bfloat16)
    return jnp.dot(exact, high, preferred_element_type=jnp.float32) + jnp.dot(
        exact, low, preferred_element_type=jnp.float32
    )


class Chunk:
    def __init__(self, index, place, start, tiles, refs):
        self.index, self.axis, self.start, self.tiles = index, index % 2, start, tiles
        self.width = tiles * LANES
        for name, ref in zip(CHUNK_REFS, refs):
            setattr(self, name, ref.at[place])


def kernel(
    slabs, reach,
    widths_hbm, owner_hbm, signs_hbm, band_ref, out_ref,
    widths_ref, owner_ref, signs_ref,
    mix, chosen, scale, *rest,
):
    wide_refs, rest = rest[:len(CHUNK_REFS)], rest[len(CHUNK_REFS):]
    narrow_refs, rest = rest[:len(CHUNK_REFS)], rest[len(CHUNK_REFS):]
    small_sem, load_sem, send1, recv1, send2, recv2, send3, recv3, near = rest
    my_group = lax.axis_index("band")
    my_slab = lax.axis_index("gslab")
    my_core = lax.rem(my_group, 2)
    bits = (my_group // 4, lax.rem(my_group // 2, 2))
    per_slice, local_bands = signs_ref.shape
    slices = widths_ref.shape[0]
    packed = mix.shape[0]
    live = reach * per_slice
    peers = 4 * slabs
    mine = out_ref.shape[0]
    extra = mine - HALF
    tall_block = mine * slabs
    row_tiles = slabs - 1
    chunks = []
    start = 0
    for refs, tiles in ((wide_refs, 2), (narrow_refs, 1)):
        for place in range(refs[0].shape[0]):
            chunks.append(Chunk(len(chunks), place, start, tiles, refs))
            start += tiles * LANES
    quarter_columns = start
    count = len(chunks)

    def group_of(axis, along, other, core):
        return along * 4 + other * 2 + core if axis == 0 else other * 4 + along * 2 + core

    def own(axis):
        return bits[axis], bits[1 - axis]

    def here_at(axis):
        return own(axis)[0] * 2 + my_core

    def quarter_at(axis, k):
        return lax.rem(own(axis)[0] * 2 + 2 + k // 2 * 2, 4) + lax.rem(my_core + k + k // 2, 2)

    def load(chunk, quarter):
        start = quarter * quarter_columns + chunk.start
        return pltpu.make_async_copy(
            band_ref.at[:, pl.ds(pl.multiple_of(start, LANES), chunk.width)],
            chunk.held.at[quarter],
            load_sem.at[chunk.index % 3],
        )

    def load_chunk(chunk):
        for quarter in range(4):
            load(chunk, quarter).start()

    def wait_bytes(ref, semaphore):
        pltpu.make_async_copy(ref, ref, semaphore).wait()

    small = [
        pltpu.make_async_copy(signs_hbm, signs_ref, small_sem.at[0]),
        pltpu.make_async_copy(widths_hbm, widths_ref, small_sem.at[1]),
        pltpu.make_async_copy(owner_hbm, owner_ref, small_sem.at[2]),
    ]
    for copy in small:
        copy.start()
    load_chunk(chunks[0])

    barrier = pltpu.get_barrier_semaphore()

    def greet(semaphore, group, slab):
        pl.semaphore_signal(
            semaphore, inc=1, device_id={"band": group, "gslab": slab}, device_id_type=MESH
        )

    inner = lax.rem(my_slab + slabs - 1, slabs) // row_tiles
    outer = my_slab // row_tiles
    sides = 2 - inner - outer

    def greet_sides(semaphore):
        @pl.when(my_slab > 0)
        def _():
            greet(semaphore, my_group, my_slab - 1)

        @pl.when(my_slab < slabs - 1)
        def _():
            greet(semaphore, my_group, my_slab + 1)

    greet(barrier, group_of(0, bits[0], bits[1], 1 - my_core), my_slab)
    for axis in range(2):
        along, other = own(axis)
        for core in range(2):
            greet(barrier, group_of(axis, 1 - along, other, core), my_slab)
    greet_sides(barrier)
    load_chunk(chunks[1])
    for copy in small:
        copy.wait()

    ends = []
    running = jnp.int32(0)
    for s in range(slices):
        running = running + widths_ref[s]
        ends.append(running)

    first_band = my_group * local_bands
    bands = first_band + lax.broadcasted_iota(jnp.int32, (1, local_bands), 1)
    slice_of = jnp.zeros((1, local_bands), jnp.int32)
    first = jnp.int32(0)
    for s in range(slices):
        slice_of = slice_of + jnp.where(bands >= ends[s], 1, 0)
        first = first + jnp.where(first_band >= ends[s], 1, 0)
    row = lax.broadcasted_iota(jnp.int32, (packed, per_slice), 0)
    column = lax.broadcasted_iota(jnp.int32, (packed, per_slice), 1)
    repeat = jnp.where(lax.rem(row, per_slice) == column, 1.0, 0.0).astype(jnp.float32)
    signs = jnp.dot(
        repeat, signs_ref[...].astype(jnp.float32), preferred_element_type=jnp.float32
    )
    row = lax.broadcasted_iota(jnp.int32, (packed, local_bands), 0)
    hit = (slice_of - first == row // per_slice) & (row < live)
    mix[...] = jnp.where(hit, signs, 0.0).astype(jnp.bfloat16)

    def exchange(chunk, quarter, source):
        return pltpu.make_async_remote_copy(
            src_ref=chunk.sent.at[quarter],
            dst_ref=chunk.got.at[source],
            send_sem=send1,
            recv_sem=recv1.at[chunk.index],
            device_id={
                "band": group_of(chunk.axis, quarter // 2, own(chunk.axis)[1], lax.rem(quarter, 2)),
                "gslab": my_slab,
            },
            device_id_type=MESH,
        )

    def partial_sums(chunk, quarter):
        sums = two_term_dot(mix[...], chunk.held[quarter])
        return sums[:live].reshape(live // HALF, HALF, chunk.width)

    def ready(chunk):
        if chunk.index + 2 < count:
            load_chunk(chunks[chunk.index + 2])
        wait_bytes(chunk.held, load_sem.at[chunk.index % 3])

    def send_partial(chunk, first=0, last=4):
        here = here_at(chunk.axis)

        @pl.loop(first, min(last, 3))
        def _(k):
            quarter = quarter_at(chunk.axis, k)
            chunk.sent[quarter] = partial_sums(chunk, quarter)
            exchange(chunk, quarter, here).start()

        if last == 4:
            chunk.got[here] = partial_sums(chunk, here)

    def cross(chunk):
        along, other = own(chunk.axis)
        return pltpu.make_async_remote_copy(
            src_ref=chunk.half.at[0],
            dst_ref=chunk.came,
            send_sem=send2,
            recv_sem=recv2.at[chunk.index],
            device_id={"band": group_of(chunk.axis, along, 1 - other, my_core), "gslab": my_slab},
            device_id_type=MESH,
        )

    def merge(chunk):
        wait_bytes(chunk.got.at[pl.ds(0, 3)], recv1.at[chunk.index])
        rows = chunk.got[...].reshape(4 * live, chunk.width)
        value = two_term_dot(chosen[chunk.axis], rows)
        chunk.half[...] = value.reshape(2, peers * mine, chunk.width)
        cross(chunk).start()

    def deliver(chunk, slab, quarter):
        return pltpu.make_async_remote_copy(
            src_ref=chunk.done.at[quarter * slabs + slab],
            dst_ref=chunk.parcel.at[my_slab, here_at(chunk.axis)],
            send_sem=send3,
            recv_sem=recv3.at[chunk.index],
            device_id={
                "band": group_of(chunk.axis, quarter // 2, own(chunk.axis)[1], lax.rem(quarter, 2)),
                "gslab": slab,
            },
            device_id_type=MESH,
        )

    def finish(chunk):
        here = here_at(chunk.axis)
        cross(chunk).wait_recv()
        total = (chunk.half[1] + chunk.came[...]) * scale[chunk.axis, :, :1]
        total = total.reshape(4 * row_tiles, SUBLANES, chunk.width)
        level = lax.broadcasted_iota(jnp.int32, (SUBLANES, LANES), 0)
        early = level % HALF < extra
        for peer in range(peers if chunk.tiles == 1 else 0):
            quarter, slab = divmod(peer, slabs)
            tile = [total[quarter * row_tiles + k] for k in range(row_tiles)]
            for at in range(0, HALF, extra):
                place = slab % 2 * HALF + at
                chunk.done[peer, at // extra] = tile[slab // 2][place:place + extra]
            chunk.done[peer, HALF // extra] = tile[-1][slab * extra:(slab + 1) * extra]
        for quarter in range(4 if chunk.tiles == 2 else 0):
            tile = [total[quarter * row_tiles + k] for k in range(row_tiles)]
            left = [t[:, :LANES] for t in tile]
            right = [t[:, LANES:] for t in tile]
            even = jnp.where(early, left[-1], pltpu.roll(right[-1], extra, 0))
            odd = jnp.where(early, pltpu.roll(left[-1], SUBLANES - extra, 0), right[-1])
            for slab in range(slabs):
                at = slab % 2 * HALF
                end = slab // 2 * HALF
                peer = quarter * slabs + slab
                chunk.done[peer, 0] = left[slab // 2][at:at + HALF]
                chunk.done[peer, 1] = right[slab // 2][at:at + HALF]
                chunk.done[peer, 2] = (odd if slab % 2 else even)[end:end + HALF]
        pltpu.make_async_copy(
            chunk.done.at[here * slabs + my_slab],
            chunk.parcel.at[my_slab, here],
            recv3.at[chunk.index],
        ).start()
        side = my_slab // 2

        @pl.loop(0, 8)
        def _(k):
            deliver(chunk, 2 - 2 * side + k // 4, lax.rem(here + k, 4)).start()

        @pl.loop(0, 4)
        def _(k):
            deliver(chunk, 4 * side + 1 - my_slab, lax.rem(here + k, 4)).start()

        @pl.loop(1, 4)
        def _(k):
            deliver(chunk, my_slab, lax.rem(here + k, 4)).start()

    def unpack(chunk):
        wait_bytes(chunk.parcel, recv3.at[chunk.index])
        for slab in range(slabs):
            for quarter in range(4):
                at = (slab * 4 + quarter) * quarter_columns + chunk.start
                if chunk.tiles == 1:
                    columns = slice(at, at + LANES)
                    for piece in range(mine // extra):
                        rows = slice(piece * extra, (piece + 1) * extra)
                        out_ref[rows, columns] = chunk.parcel[slab, quarter, piece]
                    continue
                for tile in range(2):
                    columns = slice(at + tile * LANES, at + (tile + 1) * LANES)
                    out_ref[:HALF, columns] = chunk.parcel[slab, quarter, tile]
                    out_ref[HALF:, columns] = chunk.parcel[
                        slab, quarter, 2, tile * extra:(tile + 1) * extra
                    ]

    lead, second = chunks[:2]
    ready(lead)

    @pl.loop(0, 2)
    def _(k):
        quarter = quarter_at(0, k)
        lead.sent[quarter] = partial_sums(lead, quarter)

    pl.semaphore_wait(barrier, 5 + sides)

    @pl.loop(0, 2)
    def _(k):
        exchange(lead, quarter_at(0, k), here_at(0)).start()

    ready(second)
    send_partial(second, 0, 2)
    send_partial(lead, 2, 4)
    send_partial(second, 2, 4)
    greet_sides(near.at[0])

    for axis in range(2):
        along, other = own(axis)
        shape = (2 * peers * mine, 1)
        tall = lax.broadcasted_iota(jnp.int32, shape, 0)
        stays = tall // (peers * mine)
        rest = lax.rem(tall, peers * mine)
        quarter = rest // tall_block
        rest = lax.rem(rest, tall_block)
        low = rest < slabs * HALF
        beyond = rest - slabs * HALF
        slab = jnp.where(low, rest // HALF, beyond // extra)
        within = jnp.where(low, lax.rem(rest, HALF), HALF + lax.rem(beyond, extra))
        side = jnp.where(stays == 1, other, 1 - other)
        group = group_of(axis, quarter // 2, side, lax.rem(quarter, 2))
        output_row = (group * slabs + slab) * mine + within
        block = output_row // per_slice
        target = jnp.zeros(shape, jnp.int32)
        for s in range(slices):
            target = jnp.where(block == s, owner_ref[s], target)
        breadth = jnp.ones(shape, jnp.int32)
        for s in range(slices):
            breadth = jnp.where(target == s, widths_ref[s], breadth)
        root = 1.0 / jnp.sqrt(breadth.astype(jnp.float32))
        scale[axis] = jnp.broadcast_to(root[peers * mine:], (peers * mine, LANES))
        wanted = target * per_slice + lax.rem(output_row, per_slice)
        wide = lax.broadcasted_iota(jnp.int32, (1, 4 * live), 1)
        place = lax.rem(wide, live)
        quarter = wide // live
        begin = group_of(axis, quarter // 2, other, lax.rem(quarter, 2)) * local_bands
        lowest = jnp.zeros((1, 4 * live), jnp.int32)
        for s in range(slices):
            lowest = lowest + jnp.where(begin >= ends[s], 1, 0)
        offered = lowest * per_slice + place
        chosen[axis] = jnp.where(wanted == offered, 1.0, 0.0).astype(jnp.bfloat16)

    known = 0

    def learn():
        pl.semaphore_wait(near.at[known], sides)
        if known + 1 < row_tiles:
            greet_sides(near.at[known + 1])

    for step in range(2, count + UNPACK_LAG):
        if step < count:
            ready(chunks[step])
            send_partial(chunks[step])
        if known < row_tiles:
            learn()
            known += 1
        if 0 <= step - MERGE_LAG < count:
            merge(chunks[step - MERGE_LAG])
        if 0 <= step - FINISH_LAG < count:
            finish(chunks[step - FINISH_LAG])
        if 0 <= step - UNPACK_LAG < count:
            unpack(chunks[step - UNPACK_LAG])

    for refs in (wide_refs, narrow_refs):
        named = dict(zip(CHUNK_REFS, refs))
        wait_bytes(named["sent"].at[:, pl.ds(0, 3)], send1)
        wait_bytes(named["came"], send2)
        wait_bytes(named["done"].at[:, pl.ds(0, peers - 1)], send3)


def on_device(groups, slabs, band_coeffs, sign_table, slice_widths, owner_map):
    local_bands, local_columns = band_coeffs.shape
    per_slice = sign_table.shape[0]
    rows = owner_map.shape[0] * per_slice
    tiles, odd = divmod(local_columns, 4 * LANES)
    mine = rows // (8 * slabs)
    reach = (local_bands - 2) // NARROWEST + 2
    live = reach * per_slice
    fits = 2 * (mine - HALF) == HALF and slabs == HALF and live % HALF == 0
    if groups != 8 or odd or rows % (8 * slabs) or not fits or tiles % 2 or tiles <= NARROW:
        return dense(band_coeffs, sign_table, slice_widths, owner_map)
    peers = 4 * slabs
    extra = mine - HALF

    def buffers(count, tiles):
        width = tiles * LANES
        block = (mine * tiles // HALF, HALF, LANES) if tiles == 2 else (mine // extra, extra, LANES)
        return [
            pltpu.VMEM((count, 4, local_bands, width), jnp.float32),
            pltpu.VMEM((count, 4, live // HALF, HALF, width), jnp.float32),
            pltpu.VMEM((count, 4, live // HALF, HALF, width), jnp.float32),
            pltpu.VMEM((count, 2, peers * mine, width), jnp.float32),
            pltpu.VMEM((count, peers * mine, width), jnp.float32),
            pltpu.VMEM((count, peers, *block), jnp.float32),
            pltpu.VMEM((count, slabs, 4, *block), jnp.float32),
        ]

    wide = (tiles - NARROW) // 2
    count = wide + NARROW
    return pl.pallas_call(
        functools.partial(kernel, slabs, reach),
        out_shape=pltpu.VMEM((mine, local_columns * slabs), jnp.float32),
        in_specs=[pl.BlockSpec(memory_space=pl.ANY)] * 4,
        out_specs=pl.BlockSpec(memory_space=pltpu.VMEM),
        scratch_shapes=[
            pltpu.SMEM(slice_widths.shape, jnp.int32),
            pltpu.SMEM(owner_map.shape, jnp.int32),
            pltpu.VMEM(sign_table.shape, jnp.int32),
            pltpu.VMEM((-(-live // SUBLANES) * SUBLANES, local_bands), jnp.bfloat16),
            pltpu.VMEM((2, 2 * peers * mine, 4 * live), jnp.bfloat16),
            pltpu.VMEM((2, peers * mine, LANES), jnp.float32),
            *buffers(wide, 2),
            *buffers(NARROW, 1),
            pltpu.SemaphoreType.DMA((3,)),
            pltpu.SemaphoreType.DMA((3,)),
            pltpu.SemaphoreType.DMA,
            pltpu.SemaphoreType.DMA((count,)),
            pltpu.SemaphoreType.DMA,
            pltpu.SemaphoreType.DMA((count,)),
            pltpu.SemaphoreType.DMA,
            pltpu.SemaphoreType.DMA((count,)),
            pltpu.SemaphoreType.REGULAR((slabs - 1,)),
        ],
        compiler_params=pltpu.CompilerParams(
            collective_id=0,
            has_side_effects=True,
            vmem_limit_bytes=VMEM - SUBLANES * local_columns * slabs * 4,
        ),
        name="pseudobands",
    )(slice_widths, owner_map, sign_table, band_coeffs)


def solution(mesh):
    return jax.shard_map(
        functools.partial(on_device, mesh.shape["band"], mesh.shape["gslab"]),
        mesh=mesh,
        in_specs=(P("band", "gslab"), P(None, "band"), P(), P()),
        out_specs=P(("band", "gslab"), None),
        check_vma=False,
    )
```

```python
import functools

import jax
import jax.numpy as jnp
from jax import lax
from jax.experimental import pallas as pl
from jax.experimental.pallas import tpu as pltpu
from jax.sharding import PartitionSpec as P

NARROWEST = 96
LANES = 128
SUBLANES = 8
HALF = 4
VMEM = 67043328
COMMON_REFS = ("held", "half", "came", "done", "parcel", "sent", "got")
LEAD = 2
CHUNK_REFS = (COMMON_REFS, *[COMMON_REFS + ("keep", "give", "take")] * 2)
NARROW = 2
MERGE_LAG = 2
NEAR_LAG = 3
FAR_LAG = 4
FINISH_LAG = 6
UNPACK_LAG = 8
MESH = pl.DeviceIdType.MESH


def mixing_rows(row_ids, slice_of_band, sign_float, owner_map, inverse, per_slice):
    slice_count = owner_map.shape[0]
    slot_group = row_ids // per_slice
    within = row_ids % per_slice
    slice_range = jnp.arange(slice_count, dtype=jnp.int32)
    picked = slot_group[:, None] == slice_range[None, :]
    target = jnp.sum(jnp.where(picked, owner_map[None, :], 0), axis=1)
    member = target[:, None] == slice_range[None, :]
    row_scale = jnp.sum(jnp.where(member, inverse[None, :], 0.0), axis=1)
    one_hot = (within[:, None] == jnp.arange(per_slice, dtype=jnp.int32)[None, :]).astype(
        jnp.float32
    )
    sign_rows = jnp.dot(
        one_hot, sign_float, precision=lax.Precision.HIGHEST, preferred_element_type=jnp.float32
    )
    return jnp.where(slice_of_band[None, :] == target[:, None], sign_rows * row_scale[:, None], 0.0)


def dense(band_coeffs, sign_table, slice_widths, owner_map):
    local_bands = band_coeffs.shape[0]
    per_slice = sign_table.shape[0]
    slice_count = owner_map.shape[0]
    total_rows = slice_count * per_slice
    first_band = lax.axis_index("band") * local_bands
    band_ids = first_band + jnp.arange(local_bands, dtype=jnp.int32)
    ends = jnp.cumsum(slice_widths)
    slice_of_band = jnp.sum((band_ids[:, None] >= ends[None, :]).astype(jnp.int32), axis=1)
    inverse = 1.0 / jnp.sqrt(slice_widths.astype(jnp.float32))
    sign_float = sign_table.astype(jnp.float32)
    row_ids = jnp.arange(total_rows, dtype=jnp.int32)
    mixing = mixing_rows(row_ids, slice_of_band, sign_float, owner_map, inverse, per_slice)
    summed = lax.psum_scatter(
        jnp.dot(
            mixing, band_coeffs, precision=lax.Precision.HIGHEST, preferred_element_type=jnp.float32
        ),
        "band",
        scatter_dimension=0,
        tiled=True,
    )
    return lax.all_to_all(summed, "gslab", split_axis=0, concat_axis=1, tiled=True)


def two_term_dot(exact, values):
    high = values.astype(jnp.bfloat16)
    low = (values - high.astype(jnp.float32)).astype(jnp.bfloat16)
    return jnp.dot(exact, high, preferred_element_type=jnp.float32) + jnp.dot(
        exact, low, preferred_element_type=jnp.float32
    )


class Chunk:
    def __init__(self, index, place, start, tiles, names, refs):
        self.index, self.axis, self.start, self.tiles = index, index % 2, start, tiles
        self.width = tiles * LANES
        for name, ref in zip(names, refs):
            setattr(self, name, ref.at[place])


def kernel(
    slabs, reach, chip_reach,
    widths_hbm, owner_hbm, signs_hbm, band_ref, out_ref,
    widths_ref, owner_ref, signs_ref,
    mix, chip_mix, chosen, chip_chosen, scale, *rest,
):
    groups = []
    for names in CHUNK_REFS:
        groups.append(rest[:len(names)])
        rest = rest[len(names):]
    small_sem, load_sem, send1, recv1, send2, recv2, send3, recv3, pair_sem, near = rest
    my_group = lax.axis_index("band")
    my_slab = lax.axis_index("gslab")
    my_core = lax.rem(my_group, 2)
    bits = (my_group // 4, lax.rem(my_group // 2, 2))
    per_slice, local_bands = signs_ref.shape
    slices = widths_ref.shape[0]
    live, chip_live = reach * per_slice, chip_reach * per_slice
    peers = 4 * slabs
    mine = out_ref.shape[0]
    extra = mine - HALF
    tall_block = mine * slabs
    row_tiles = slabs - 1
    chunks = []
    start = 0
    for names, refs, tiles in zip(CHUNK_REFS, groups, (2, 2, 1)):
        for place in range(refs[0].shape[0]):
            chunks.append(Chunk(len(chunks), place, start, tiles, names, refs))
            start += tiles * LANES
    quarter_columns = start
    count = len(chunks)

    def group_of(axis, along, other, core):
        return along * 4 + other * 2 + core if axis == 0 else other * 4 + along * 2 + core

    def own(axis):
        return bits[axis], bits[1 - axis]

    def here_at(axis):
        return own(axis)[0] * 2 + my_core

    def quarter_at(axis, k):
        return lax.rem(own(axis)[0] * 2 + 2 + k // 2 * 2, 4) + lax.rem(my_core + k + k // 2, 2)

    def load(chunk, quarter):
        start = quarter * quarter_columns + chunk.start
        return pltpu.make_async_copy(
            band_ref.at[:, pl.ds(pl.multiple_of(start, LANES), chunk.width)],
            chunk.held.at[quarter],
            load_sem.at[chunk.index % 3],
        )

    def load_chunk(chunk):
        for quarter in range(4):
            load(chunk, quarter).start()

    def wait_bytes(ref, semaphore):
        pltpu.make_async_copy(ref, ref, semaphore).wait()

    small = [
        pltpu.make_async_copy(signs_hbm, signs_ref, small_sem.at[0]),
        pltpu.make_async_copy(widths_hbm, widths_ref, small_sem.at[1]),
        pltpu.make_async_copy(owner_hbm, owner_ref, small_sem.at[2]),
    ]
    for copy in small:
        copy.start()
    load_chunk(chunks[0])

    barrier = pltpu.get_barrier_semaphore()

    def greet(semaphore, group, slab):
        pl.semaphore_signal(
            semaphore, inc=1, device_id={"band": group, "gslab": slab}, device_id_type=MESH
        )

    inner = lax.rem(my_slab + slabs - 1, slabs) // row_tiles
    outer = my_slab // row_tiles
    sides = 2 - inner - outer

    def greet_sides(semaphore):
        @pl.when(my_slab > 0)
        def _():
            greet(semaphore, my_group, my_slab - 1)

        @pl.when(my_slab < slabs - 1)
        def _():
            greet(semaphore, my_group, my_slab + 1)

    greet(barrier, group_of(0, bits[0], bits[1], 1 - my_core), my_slab)
    for axis in range(2):
        along, other = own(axis)
        for core in range(2):
            greet(barrier, group_of(axis, 1 - along, other, core), my_slab)
    greet_sides(barrier)
    load_chunk(chunks[1])
    for copy in small:
        copy.wait()

    ends = []
    running = jnp.int32(0)
    for s in range(slices):
        running = running + widths_ref[s]
        ends.append(running)

    first_band = my_group * local_bands
    bands = first_band + lax.broadcasted_iota(jnp.int32, (1, local_bands), 1)
    slice_of = jnp.zeros((1, local_bands), jnp.int32)
    for s in range(slices):
        slice_of = slice_of + jnp.where(bands >= ends[s], 1, 0)

    def fill(target, band, extent):
        first = jnp.int32(0)
        for s in range(slices):
            first = first + jnp.where(band >= ends[s], 1, 0)
        packed = target.shape[0]
        row = lax.broadcasted_iota(jnp.int32, (packed, per_slice), 0)
        column = lax.broadcasted_iota(jnp.int32, (packed, per_slice), 1)
        repeat = jnp.where(lax.rem(row, per_slice) == column, 1.0, 0.0).astype(jnp.float32)
        signs = jnp.dot(
            repeat, signs_ref[...].astype(jnp.float32), preferred_element_type=jnp.float32
        )
        row = lax.broadcasted_iota(jnp.int32, (packed, local_bands), 0)
        hit = (slice_of - first == row // per_slice) & (row < extent)
        target[...] = jnp.where(hit, signs, 0.0).astype(jnp.bfloat16)

    fill(mix, first_band, live)

    def exchange(chunk, quarter, source):
        return pltpu.make_async_remote_copy(
            src_ref=chunk.sent.at[quarter],
            dst_ref=chunk.got.at[source],
            send_sem=send1,
            recv_sem=recv1.at[chunk.index],
            device_id={
                "band": group_of(chunk.axis, quarter // 2, own(chunk.axis)[1], lax.rem(quarter, 2)),
                "gslab": my_slab,
            },
            device_id_type=MESH,
        )

    def partial_sums(chunk, quarter):
        sums = two_term_dot(mix[...], chunk.held[quarter])
        return sums[:live].reshape(live // HALF, HALF, chunk.width)

    def chip_sums(chunk, quarter):
        sums = two_term_dot(chip_mix[...], chunk.held[quarter])
        return sums[:chip_live].reshape(chip_live // HALF, HALF, chunk.width)

    def pair(chunk, k):
        return pltpu.make_async_remote_copy(
            src_ref=chunk.give.at[k],
            dst_ref=chunk.take.at[k],
            send_sem=send1,
            recv_sem=pair_sem.at[chunk.index - LEAD],
            device_id={"band": my_group + 1 - 2 * my_core, "gslab": my_slab},
            device_id_type=MESH,
        )

    def pair_partial(chunk):
        along = own(chunk.axis)[0]

        @pl.loop(0, 2)
        def _(k):
            side = lax.rem(along + 1 + k, 2)
            chunk.give[k] = chip_sums(chunk, side * 2 + 1 - my_core)
            pair(chunk, k).start()

        @pl.loop(0, 2)
        def _(k):
            side = lax.rem(along + 1 + k, 2)
            chunk.keep[k] = chip_sums(chunk, side * 2 + my_core)

    def across(chunk):
        along, other = own(chunk.axis)
        return pltpu.make_async_remote_copy(
            src_ref=chunk.sent,
            dst_ref=chunk.got.at[along],
            send_sem=send1,
            recv_sem=recv1.at[chunk.index],
            device_id={"band": group_of(chunk.axis, 1 - along, other, my_core), "gslab": my_slab},
            device_id_type=MESH,
        )

    def fold(chunk):
        wait_bytes(chunk.take, pair_sem.at[chunk.index - LEAD])
        chunk.sent[...] = chunk.keep[0] + chunk.take[0]
        across(chunk).start()
        chunk.got[own(chunk.axis)[0]] = chunk.keep[1] + chunk.take[1]

    def ready(chunk):
        if chunk.index + 2 < count:
            load_chunk(chunks[chunk.index + 2])
        wait_bytes(chunk.held, load_sem.at[chunk.index % 3])

    def send_partial(chunk, first=0, last=4):
        here = here_at(chunk.axis)

        @pl.loop(first, min(last, 3))
        def _(k):
            quarter = quarter_at(chunk.axis, k)
            chunk.sent[quarter] = partial_sums(chunk, quarter)
            exchange(chunk, quarter, here).start()

        if last == 4:
            chunk.got[here] = partial_sums(chunk, here)

    def side_of(far):
        return 1 - my_slab // 2 if far else my_slab // 2

    def rows_of(far):
        return pl.ds(pl.multiple_of(side_of(far) * (2 * tall_block), SUBLANES), 2 * tall_block)

    def cross(chunk, far):
        along, other = own(chunk.axis)
        return pltpu.make_async_remote_copy(
            src_ref=chunk.half.at[0, rows_of(far)],
            dst_ref=chunk.came.at[rows_of(far)],
            send_sem=send2,
            recv_sem=recv2.at[2 * chunk.index + far],
            device_id={"band": group_of(chunk.axis, along, 1 - other, my_core), "gslab": my_slab},
            device_id_type=MESH,
        )

    def merge(chunk):
        if chunk.index < LEAD:
            wait_bytes(chunk.got.at[pl.ds(0, 3)], recv1.at[chunk.index])
            rows = chunk.got[...].reshape(4 * live, chunk.width)
            value = two_term_dot(chosen[chunk.axis], rows)
        else:
            wait_bytes(chunk.got.at[0], recv1.at[chunk.index])
            rows = chunk.got[...].reshape(2 * chip_live, chunk.width)
            value = two_term_dot(chip_chosen[chunk.axis], rows)
        chunk.half[...] = value.reshape(2, peers * mine, chunk.width)
        cross(chunk, 1).start()

    def deliver(chunk, far, place):
        side = side_of(far)
        quarter = place // 2
        return pltpu.make_async_remote_copy(
            src_ref=chunk.done.at[side * (peers // 2) + place],
            dst_ref=chunk.parcel.at[my_slab, here_at(chunk.axis)],
            send_sem=send3,
            recv_sem=recv3.at[chunk.index],
            device_id={
                "band": group_of(chunk.axis, quarter // 2, own(chunk.axis)[1], lax.rem(quarter, 2)),
                "gslab": 2 * side + lax.rem(place, 2),
            },
            device_id_type=MESH,
        )

    def finish(chunk, far):
        here = here_at(chunk.axis)
        cross(chunk, far).wait_recv()
        rows = rows_of(far)
        total = (chunk.half[1, rows] + chunk.came[rows]) * scale[chunk.axis, rows, :1]
        total = total.reshape(2 * row_tiles, SUBLANES, chunk.width)
        level = lax.broadcasted_iota(jnp.int32, (SUBLANES, LANES), 0)
        early = level % HALF < extra
        first = side_of(far) * (peers // 2)
        for group in range(2):
            tile = [total[group * row_tiles + k] for k in range(row_tiles)]
            if chunk.tiles == 1:
                for place in range(slabs):
                    peer = first + group * slabs + place
                    for at in range(0, HALF, extra):
                        row = place % 2 * HALF + at
                        chunk.done[peer, at // extra] = tile[place // 2][row:row + extra]
                    chunk.done[peer, HALF // extra] = tile[-1][place * extra:(place + 1) * extra]
                continue
            left = [t[:, :LANES] for t in tile]
            right = [t[:, LANES:] for t in tile]
            even = jnp.where(early, left[-1], pltpu.roll(right[-1], extra, 0))
            odd = jnp.where(early, pltpu.roll(left[-1], SUBLANES - extra, 0), right[-1])
            for place in range(slabs):
                at = place % 2 * HALF
                end = place // 2 * HALF
                peer = first + group * slabs + place
                chunk.done[peer, 0] = left[place // 2][at:at + HALF]
                chunk.done[peer, 1] = right[place // 2][at:at + HALF]
                chunk.done[peer, 2] = (odd if place % 2 else even)[end:end + HALF]
        myself = here * 2 + lax.rem(my_slab, 2)
        if far:
            @pl.loop(0, 8)
            def _(k):
                deliver(chunk, 1, lax.rem(myself + k, 8)).start()
        else:
            pltpu.make_async_copy(
                chunk.done.at[first + myself], chunk.parcel.at[my_slab, here], recv3.at[chunk.index]
            ).start()

            @pl.loop(1, 8)
            def _(k):
                deliver(chunk, 0, lax.rem(myself + k, 8)).start()

    def unpack(chunk):
        wait_bytes(chunk.parcel, recv3.at[chunk.index])
        for slab in range(slabs):
            for quarter in range(4):
                at = (slab * 4 + quarter) * quarter_columns + chunk.start
                if chunk.tiles == 1:
                    columns = slice(at, at + LANES)
                    for piece in range(mine // extra):
                        rows = slice(piece * extra, (piece + 1) * extra)
                        out_ref[rows, columns] = chunk.parcel[slab, quarter, piece]
                    continue
                for tile in range(2):
                    columns = slice(at + tile * LANES, at + (tile + 1) * LANES)
                    out_ref[:HALF, columns] = chunk.parcel[slab, quarter, tile]
                    out_ref[HALF:, columns] = chunk.parcel[
                        slab, quarter, 2, tile * extra:(tile + 1) * extra
                    ]

    lead, second = chunks[:2]
    ready(lead)

    @pl.loop(0, 2)
    def _(k):
        quarter = quarter_at(0, k)
        lead.sent[quarter] = partial_sums(lead, quarter)

    pl.semaphore_wait(barrier, 5 + sides)

    @pl.loop(0, 2)
    def _(k):
        exchange(lead, quarter_at(0, k), here_at(0)).start()

    ready(second)
    send_partial(second, 0, 2)
    send_partial(lead, 2, 4)
    send_partial(second, 2, 4)
    greet_sides(near.at[0])
    fill(chip_mix, (my_group - my_core) * local_bands, chip_live)
    ready(chunks[LEAD])
    pair_partial(chunks[LEAD])

    for axis in range(2):
        along, other = own(axis)
        shape = (2 * peers * mine, 1)
        tall = lax.broadcasted_iota(jnp.int32, shape, 0)
        stays = tall // (peers * mine)
        rest = lax.rem(tall, peers * mine)
        part = rest // tall_block
        rest = lax.rem(rest, tall_block)
        low = rest < slabs * HALF
        beyond = rest - slabs * HALF
        place = jnp.where(low, rest // HALF, beyond // extra)
        quarter = lax.rem(part, 2) * 2 + place // 2
        slab = part // 2 * 2 + lax.rem(place, 2)
        within = jnp.where(low, lax.rem(rest, HALF), HALF + lax.rem(beyond, extra))
        side = jnp.where(stays == 1, other, 1 - other)
        group = group_of(axis, quarter // 2, side, lax.rem(quarter, 2))
        output_row = (group * slabs + slab) * mine + within
        block = output_row // per_slice
        target = jnp.zeros(shape, jnp.int32)
        for s in range(slices):
            target = jnp.where(block == s, owner_ref[s], target)
        breadth = jnp.ones(shape, jnp.int32)
        for s in range(slices):
            breadth = jnp.where(target == s, widths_ref[s], breadth)
        root = 1.0 / jnp.sqrt(breadth.astype(jnp.float32))
        scale[axis] = jnp.broadcast_to(root[peers * mine:], (peers * mine, LANES))
        wanted = target * per_slice + lax.rem(output_row, per_slice)
        for target, cores, extent in ((chosen, 2, live), (chip_chosen, 1, chip_live)):
            wide = lax.broadcasted_iota(jnp.int32, (1, 2 * cores * extent), 1)
            place = lax.rem(wide, extent)
            source = wide // extent
            begin = group_of(axis, source // cores, other, lax.rem(source, cores)) * local_bands
            lowest = jnp.zeros(wide.shape, jnp.int32)
            for s in range(slices):
                lowest = lowest + jnp.where(begin >= ends[s], 1, 0)
            offered = lowest * per_slice + place
            target[axis] = jnp.where(wanted == offered, 1.0, 0.0).astype(jnp.bfloat16)

    known = 0

    def learn():
        pl.semaphore_wait(near.at[known], sides)
        if known + 1 < row_tiles:
            greet_sides(near.at[known + 1])

    for step in range(LEAD, count + UNPACK_LAG):
        if step < count:
            fold(chunks[step])
        if step + 1 < count:
            ready(chunks[step + 1])
            pair_partial(chunks[step + 1])
        if known < row_tiles:
            learn()
            known += 1
        if 0 <= step - MERGE_LAG < count:
            merge(chunks[step - MERGE_LAG])
        if 0 <= step - NEAR_LAG < count:
            cross(chunks[step - NEAR_LAG], 0).start()
        if 0 <= step - FAR_LAG < count:
            finish(chunks[step - FAR_LAG], 1)
        if 0 <= step - FINISH_LAG < count:
            finish(chunks[step - FINISH_LAG], 0)
        if 0 <= step - UNPACK_LAG < count:
            unpack(chunks[step - UNPACK_LAG])

    for names, refs in zip(CHUNK_REFS, groups):
        named = dict(zip(names, refs))
        if "give" in named:
            wait_bytes(named["give"], send1)
            wait_bytes(named["sent"], send1)
        else:
            wait_bytes(named["sent"].at[:, pl.ds(0, 3)], send1)
        wait_bytes(named["came"], send2)
        wait_bytes(named["done"].at[:, pl.ds(0, peers - 1)], send3)


def on_device(groups, slabs, band_coeffs, sign_table, slice_widths, owner_map):
    local_bands, local_columns = band_coeffs.shape
    per_slice = sign_table.shape[0]
    rows = owner_map.shape[0] * per_slice
    tiles, odd = divmod(local_columns, 4 * LANES)
    mine = rows // (8 * slabs)
    reach = (local_bands - 2) // NARROWEST + 2
    chip_reach = (2 * local_bands - 2) // NARROWEST + 2
    live, chip_live = reach * per_slice, chip_reach * per_slice
    fits = 2 * (mine - HALF) == HALF and slabs == HALF and per_slice % HALF == 0
    if groups != 8 or odd or rows % (8 * slabs) or not fits or tiles % 2 or tiles <= NARROW + 2 * LEAD:
        return dense(band_coeffs, sign_table, slice_widths, owner_map)
    peers = 4 * slabs
    extra = mine - HALF

    def buffers(count, tiles, paired):
        width = tiles * LANES
        block = (mine * tiles // HALF, HALF, LANES) if tiles == 2 else (mine // extra, extra, LANES)
        core, chip = [(rows // HALF, HALF, width) for rows in (live, chip_live)]
        shapes = [
            (4, local_bands, width),
            (2, peers * mine, width),
            (peers * mine, width),
            (peers, *block),
            (slabs, 4, *block),
        ]
        shapes += [chip, *[(2, *chip)] * 4] if paired else [(4, *core)] * 2
        return [pltpu.VMEM((count, *shape), jnp.float32) for shape in shapes]

    def aligned(rows):
        return -(-rows // SUBLANES) * SUBLANES

    wide = (tiles - NARROW) // 2 - LEAD
    count = LEAD + wide + NARROW
    return pl.pallas_call(
        functools.partial(kernel, slabs, reach, chip_reach),
        out_shape=pltpu.VMEM((mine, local_columns * slabs), jnp.float32),
        in_specs=[pl.BlockSpec(memory_space=pl.ANY)] * 4,
        out_specs=pl.BlockSpec(memory_space=pltpu.VMEM),
        scratch_shapes=[
            pltpu.SMEM(slice_widths.shape, jnp.int32),
            pltpu.SMEM(owner_map.shape, jnp.int32),
            pltpu.VMEM(sign_table.shape, jnp.int32),
            pltpu.VMEM((aligned(live), local_bands), jnp.bfloat16),
            pltpu.VMEM((aligned(chip_live), local_bands), jnp.bfloat16),
            pltpu.VMEM((2, 2 * peers * mine, 4 * live), jnp.bfloat16),
            pltpu.VMEM((2, 2 * peers * mine, 2 * chip_live), jnp.bfloat16),
            pltpu.VMEM((2, peers * mine, LANES), jnp.float32),
            *buffers(LEAD, 2, False),
            *buffers(wide, 2, True),
            *buffers(NARROW, 1, True),
            pltpu.SemaphoreType.DMA((3,)),
            pltpu.SemaphoreType.DMA((3,)),
            pltpu.SemaphoreType.DMA,
            pltpu.SemaphoreType.DMA((count,)),
            pltpu.SemaphoreType.DMA,
            pltpu.SemaphoreType.DMA((2 * count,)),
            pltpu.SemaphoreType.DMA,
            pltpu.SemaphoreType.DMA((count,)),
            pltpu.SemaphoreType.DMA((count - LEAD,)),
            pltpu.SemaphoreType.REGULAR((slabs - 1,)),
        ],
        compiler_params=pltpu.CompilerParams(
            collective_id=0,
            has_side_effects=True,
            vmem_limit_bytes=VMEM - SUBLANES * local_columns * slabs * 4,
        ),
        name="pseudobands",
    )(slice_widths, owner_map, sign_table, band_coeffs)


def solution(mesh):
    return jax.shard_map(
        functools.partial(on_device, mesh.shape["band"], mesh.shape["gslab"]),
        mesh=mesh,
        in_specs=(P("band", "gslab"), P(None, "band"), P(), P()),
        out_specs=P(("band", "gslab"), None),
        check_vma=False,
    )
```

```python
import functools

import jax
import jax.numpy as jnp
from jax import lax
from jax.experimental import pallas as pl
from jax.experimental.pallas import tpu as pltpu
from jax.sharding import PartitionSpec as P

NARROWEST = 96
LANES = 128
SUBLANES = 8
HALF = 4
VMEM = 67043328
COMMON_REFS = ("held", "half", "came", "done", "parcel", "sent", "got")
LEAD = 2
CHUNK_REFS = (COMMON_REFS, *[COMMON_REFS + ("keep", "give", "take")] * 2)
NARROW = 2
MERGE_LAG = 2
NEAR_LAG = 3
FAR_LAG = 4
FINISH_LAG = 7
UNPACK_LAG = 11
MESH = pl.DeviceIdType.MESH


def mixing_rows(row_ids, slice_of_band, sign_float, owner_map, inverse, per_slice):
    slice_count = owner_map.shape[0]
    slot_group = row_ids // per_slice
    within = row_ids % per_slice
    slice_range = jnp.arange(slice_count, dtype=jnp.int32)
    picked = slot_group[:, None] == slice_range[None, :]
    target = jnp.sum(jnp.where(picked, owner_map[None, :], 0), axis=1)
    member = target[:, None] == slice_range[None, :]
    row_scale = jnp.sum(jnp.where(member, inverse[None, :], 0.0), axis=1)
    one_hot = (within[:, None] == jnp.arange(per_slice, dtype=jnp.int32)[None, :]).astype(
        jnp.float32
    )
    sign_rows = jnp.dot(
        one_hot, sign_float, precision=lax.Precision.HIGHEST, preferred_element_type=jnp.float32
    )
    return jnp.where(slice_of_band[None, :] == target[:, None], sign_rows * row_scale[:, None], 0.0)


def dense(band_coeffs, sign_table, slice_widths, owner_map):
    local_bands = band_coeffs.shape[0]
    per_slice = sign_table.shape[0]
    slice_count = owner_map.shape[0]
    total_rows = slice_count * per_slice
    first_band = lax.axis_index("band") * local_bands
    band_ids = first_band + jnp.arange(local_bands, dtype=jnp.int32)
    ends = jnp.cumsum(slice_widths)
    slice_of_band = jnp.sum((band_ids[:, None] >= ends[None, :]).astype(jnp.int32), axis=1)
    inverse = 1.0 / jnp.sqrt(slice_widths.astype(jnp.float32))
    sign_float = sign_table.astype(jnp.float32)
    row_ids = jnp.arange(total_rows, dtype=jnp.int32)
    mixing = mixing_rows(row_ids, slice_of_band, sign_float, owner_map, inverse, per_slice)
    summed = lax.psum_scatter(
        jnp.dot(
            mixing, band_coeffs, precision=lax.Precision.HIGHEST, preferred_element_type=jnp.float32
        ),
        "band",
        scatter_dimension=0,
        tiled=True,
    )
    return lax.all_to_all(summed, "gslab", split_axis=0, concat_axis=1, tiled=True)


def two_term_dot(exact, values):
    high = values.astype(jnp.bfloat16)
    low = (values - high.astype(jnp.float32)).astype(jnp.bfloat16)
    return jnp.dot(exact, high, preferred_element_type=jnp.float32) + jnp.dot(
        exact, low, preferred_element_type=jnp.float32
    )


class Chunk:
    def __init__(self, index, place, start, tiles, names, refs):
        self.index, self.axis, self.start, self.tiles = index, index % 2, start, tiles
        self.width = tiles * LANES
        for name, ref in zip(names, refs):
            setattr(self, name, ref.at[place])


def kernel(
    slabs, reach, chip_reach,
    widths_hbm, owner_hbm, signs_hbm, band_ref, out_ref,
    widths_ref, owner_ref, signs_ref,
    mix, chip_mix, chosen, chip_chosen, scale, *rest,
):
    groups = []
    for names in CHUNK_REFS:
        groups.append(rest[:len(names)])
        rest = rest[len(names):]
    small_sem, load_sem, send1, recv1, send2, recv2, send3, recv3, pair_sem, near = rest
    my_group = lax.axis_index("band")
    my_slab = lax.axis_index("gslab")
    my_core = lax.rem(my_group, 2)
    bits = (my_group // 4, lax.rem(my_group // 2, 2))
    per_slice, local_bands = signs_ref.shape
    slices = widths_ref.shape[0]
    live, chip_live = reach * per_slice, chip_reach * per_slice
    peers = 4 * slabs
    mine = out_ref.shape[0]
    extra = mine - HALF
    tall_block = mine * slabs
    row_tiles = slabs - 1
    chunks = []
    start = 0
    for names, refs, tiles in zip(CHUNK_REFS, groups, (2, 2, 1)):
        for place in range(refs[0].shape[0]):
            chunks.append(Chunk(len(chunks), place, start, tiles, names, refs))
            start += tiles * LANES
    quarter_columns = start
    count = len(chunks)

    def group_of(axis, along, other, core):
        return along * 4 + other * 2 + core if axis == 0 else other * 4 + along * 2 + core

    def own(axis):
        return bits[axis], bits[1 - axis]

    def here_at(axis):
        return own(axis)[0] * 2 + my_core

    def quarter_at(axis, k):
        return lax.rem(own(axis)[0] * 2 + 2 + k // 2 * 2, 4) + lax.rem(my_core + k + k // 2, 2)

    def load(chunk, quarter):
        start = quarter * quarter_columns + chunk.start
        return pltpu.make_async_copy(
            band_ref.at[:, pl.ds(pl.multiple_of(start, LANES), chunk.width)],
            chunk.held.at[quarter],
            load_sem.at[chunk.index % 3],
        )

    def load_chunk(chunk):
        for quarter in range(4):
            load(chunk, quarter).start()

    def wait_bytes(ref, semaphore):
        pltpu.make_async_copy(ref, ref, semaphore).wait()

    small = [
        pltpu.make_async_copy(signs_hbm, signs_ref, small_sem.at[0]),
        pltpu.make_async_copy(widths_hbm, widths_ref, small_sem.at[1]),
        pltpu.make_async_copy(owner_hbm, owner_ref, small_sem.at[2]),
    ]
    for copy in small:
        copy.start()
    load_chunk(chunks[0])

    barrier = pltpu.get_barrier_semaphore()

    def greet(semaphore, group, slab):
        pl.semaphore_signal(
            semaphore, inc=1, device_id={"band": group, "gslab": slab}, device_id_type=MESH
        )

    inner = lax.rem(my_slab + slabs - 1, slabs) // row_tiles
    outer = my_slab // row_tiles
    sides = 2 - inner - outer

    def greet_sides(semaphore):
        @pl.when(my_slab > 0)
        def _():
            greet(semaphore, my_group, my_slab - 1)

        @pl.when(my_slab < slabs - 1)
        def _():
            greet(semaphore, my_group, my_slab + 1)

    greet(barrier, group_of(0, bits[0], bits[1], 1 - my_core), my_slab)
    for axis in range(2):
        along, other = own(axis)
        for core in range(2):
            greet(barrier, group_of(axis, 1 - along, other, core), my_slab)
    greet_sides(barrier)
    load_chunk(chunks[1])
    for copy in small:
        copy.wait()

    ends = []
    running = jnp.int32(0)
    for s in range(slices):
        running = running + widths_ref[s]
        ends.append(running)

    first_band = my_group * local_bands
    bands = first_band + lax.broadcasted_iota(jnp.int32, (1, local_bands), 1)
    slice_of = jnp.zeros((1, local_bands), jnp.int32)
    for s in range(slices):
        slice_of = slice_of + jnp.where(bands >= ends[s], 1, 0)

    def fill(target, band, extent):
        first = jnp.int32(0)
        for s in range(slices):
            first = first + jnp.where(band >= ends[s], 1, 0)
        packed = target.shape[0]
        row = lax.broadcasted_iota(jnp.int32, (packed, per_slice), 0)
        column = lax.broadcasted_iota(jnp.int32, (packed, per_slice), 1)
        repeat = jnp.where(lax.rem(row, per_slice) == column, 1.0, 0.0).astype(jnp.float32)
        signs = jnp.dot(
            repeat, signs_ref[...].astype(jnp.float32), preferred_element_type=jnp.float32
        )
        row = lax.broadcasted_iota(jnp.int32, (packed, local_bands), 0)
        hit = (slice_of - first == row // per_slice) & (row < extent)
        target[...] = jnp.where(hit, signs, 0.0).astype(jnp.bfloat16)

    fill(mix, first_band, live)

    def exchange(chunk, quarter, source):
        return pltpu.make_async_remote_copy(
            src_ref=chunk.sent.at[quarter],
            dst_ref=chunk.got.at[source],
            send_sem=send1,
            recv_sem=recv1.at[chunk.index],
            device_id={
                "band": group_of(chunk.axis, quarter // 2, own(chunk.axis)[1], lax.rem(quarter, 2)),
                "gslab": my_slab,
            },
            device_id_type=MESH,
        )

    def partial_sums(chunk, quarter):
        sums = two_term_dot(mix[...], chunk.held[quarter])
        return sums[:live].reshape(live // HALF, HALF, chunk.width)

    def chip_sums(chunk, quarter):
        sums = two_term_dot(chip_mix[...], chunk.held[quarter])
        return sums[:chip_live].reshape(chip_live // HALF, HALF, chunk.width)

    def pair(chunk, k):
        return pltpu.make_async_remote_copy(
            src_ref=chunk.give.at[k],
            dst_ref=chunk.take.at[k],
            send_sem=send1,
            recv_sem=pair_sem.at[chunk.index - LEAD],
            device_id={"band": my_group + 1 - 2 * my_core, "gslab": my_slab},
            device_id_type=MESH,
        )

    def pair_partial(chunk):
        along = own(chunk.axis)[0]

        @pl.loop(0, 2)
        def _(k):
            side = lax.rem(along + 1 + k, 2)
            chunk.give[k] = chip_sums(chunk, side * 2 + 1 - my_core)
            pair(chunk, k).start()

        @pl.loop(0, 2)
        def _(k):
            side = lax.rem(along + 1 + k, 2)
            chunk.keep[k] = chip_sums(chunk, side * 2 + my_core)

    def across(chunk):
        along, other = own(chunk.axis)
        return pltpu.make_async_remote_copy(
            src_ref=chunk.sent,
            dst_ref=chunk.got.at[along],
            send_sem=send1,
            recv_sem=recv1.at[chunk.index],
            device_id={"band": group_of(chunk.axis, 1 - along, other, my_core), "gslab": my_slab},
            device_id_type=MESH,
        )

    def fold(chunk):
        wait_bytes(chunk.take, pair_sem.at[chunk.index - LEAD])
        chunk.sent[...] = chunk.keep[0] + chunk.take[0]
        across(chunk).start()
        chunk.got[own(chunk.axis)[0]] = chunk.keep[1] + chunk.take[1]

    def ready(chunk):
        if chunk.index + 2 < count:
            load_chunk(chunks[chunk.index + 2])
        wait_bytes(chunk.held, load_sem.at[chunk.index % 3])

    def send_partial(chunk, first=0, last=4):
        here = here_at(chunk.axis)

        @pl.loop(first, min(last, 3))
        def _(k):
            quarter = quarter_at(chunk.axis, k)
            chunk.sent[quarter] = partial_sums(chunk, quarter)
            exchange(chunk, quarter, here).start()

        if last == 4:
            chunk.got[here] = partial_sums(chunk, here)

    def side_of(far):
        return 1 - my_slab // 2 if far else my_slab // 2

    def rows_of(far):
        return pl.ds(pl.multiple_of(side_of(far) * (2 * tall_block), SUBLANES), 2 * tall_block)

    def cross(chunk, far):
        along, other = own(chunk.axis)
        return pltpu.make_async_remote_copy(
            src_ref=chunk.half.at[0, rows_of(far)],
            dst_ref=chunk.came.at[rows_of(far)],
            send_sem=send2,
            recv_sem=recv2.at[2 * chunk.index + far],
            device_id={"band": group_of(chunk.axis, along, 1 - other, my_core), "gslab": my_slab},
            device_id_type=MESH,
        )

    def merge(chunk):
        if chunk.index < LEAD:
            wait_bytes(chunk.got.at[pl.ds(0, 3)], recv1.at[chunk.index])
            rows = chunk.got[...].reshape(4 * live, chunk.width)
            value = two_term_dot(chosen[chunk.axis], rows)
        else:
            wait_bytes(chunk.got.at[0], recv1.at[chunk.index])
            rows = chunk.got[...].reshape(2 * chip_live, chunk.width)
            value = two_term_dot(chip_chosen[chunk.axis], rows)
        chunk.half[...] = value.reshape(2, peers * mine, chunk.width)
        cross(chunk, 1).start()

    def deliver(chunk, far, place):
        side = side_of(far)
        quarter = place // 2
        return pltpu.make_async_remote_copy(
            src_ref=chunk.done.at[side * (peers // 2) + place],
            dst_ref=chunk.parcel.at[my_slab, here_at(chunk.axis)],
            send_sem=send3,
            recv_sem=recv3.at[chunk.index],
            device_id={
                "band": group_of(chunk.axis, quarter // 2, own(chunk.axis)[1], lax.rem(quarter, 2)),
                "gslab": 2 * side + lax.rem(place, 2),
            },
            device_id_type=MESH,
        )

    def finish(chunk, far):
        here = here_at(chunk.axis)
        cross(chunk, far).wait_recv()
        rows = rows_of(far)
        total = (chunk.half[1, rows] + chunk.came[rows]) * scale[chunk.axis, rows, :1]
        total = total.reshape(2 * row_tiles, SUBLANES, chunk.width)
        level = lax.broadcasted_iota(jnp.int32, (SUBLANES, LANES), 0)
        early = level % HALF < extra
        first = side_of(far) * (peers // 2)
        for group in range(2):
            tile = [total[group * row_tiles + k] for k in range(row_tiles)]
            if chunk.tiles == 1:
                for place in range(slabs):
                    peer = first + group * slabs + place
                    for at in range(0, HALF, extra):
                        row = place % 2 * HALF + at
                        chunk.done[peer, at // extra] = tile[place // 2][row:row + extra]
                    chunk.done[peer, HALF // extra] = tile[-1][place * extra:(place + 1) * extra]
                continue
            left = [t[:, :LANES] for t in tile]
            right = [t[:, LANES:] for t in tile]
            even = jnp.where(early, left[-1], pltpu.roll(right[-1], extra, 0))
            odd = jnp.where(early, pltpu.roll(left[-1], SUBLANES - extra, 0), right[-1])
            for place in range(slabs):
                at = place % 2 * HALF
                end = place // 2 * HALF
                peer = first + group * slabs + place
                chunk.done[peer, 0] = left[place // 2][at:at + HALF]
                chunk.done[peer, 1] = right[place // 2][at:at + HALF]
                chunk.done[peer, 2] = (odd if place % 2 else even)[end:end + HALF]
        myself = here * 2 + lax.rem(my_slab, 2)
        if far:
            @pl.loop(0, 8)
            def _(k):
                deliver(chunk, 1, lax.rem(myself + k, 8)).start()
        else:
            pltpu.make_async_copy(
                chunk.done.at[first + myself], chunk.parcel.at[my_slab, here], recv3.at[chunk.index]
            ).start()

            @pl.loop(1, 8)
            def _(k):
                deliver(chunk, 0, lax.rem(myself + k, 8)).start()

    def unpack(chunk):
        wait_bytes(chunk.parcel, recv3.at[chunk.index])
        for slab in range(slabs):
            for quarter in range(4):
                at = (slab * 4 + quarter) * quarter_columns + chunk.start
                if chunk.tiles == 1:
                    columns = slice(at, at + LANES)
                    for piece in range(mine // extra):
                        rows = slice(piece * extra, (piece + 1) * extra)
                        out_ref[rows, columns] = chunk.parcel[slab, quarter, piece]
                    continue
                for tile in range(2):
                    columns = slice(at + tile * LANES, at + (tile + 1) * LANES)
                    out_ref[:HALF, columns] = chunk.parcel[slab, quarter, tile]
                    out_ref[HALF:, columns] = chunk.parcel[
                        slab, quarter, 2, tile * extra:(tile + 1) * extra
                    ]

    lead, second = chunks[:2]
    ready(lead)

    @pl.loop(0, 2)
    def _(k):
        quarter = quarter_at(0, k)
        lead.sent[quarter] = partial_sums(lead, quarter)

    pl.semaphore_wait(barrier, 5 + sides)

    @pl.loop(0, 2)
    def _(k):
        exchange(lead, quarter_at(0, k), here_at(0)).start()

    ready(second)
    send_partial(second, 0, 2)
    send_partial(lead, 2, 4)
    send_partial(second, 2, 4)
    greet_sides(near.at[0])
    fill(chip_mix, (my_group - my_core) * local_bands, chip_live)
    ready(chunks[LEAD])
    pair_partial(chunks[LEAD])

    for axis in range(2):
        along, other = own(axis)
        shape = (2 * peers * mine, 1)
        tall = lax.broadcasted_iota(jnp.int32, shape, 0)
        stays = tall // (peers * mine)
        rest = lax.rem(tall, peers * mine)
        part = rest // tall_block
        rest = lax.rem(rest, tall_block)
        low = rest < slabs * HALF
        beyond = rest - slabs * HALF
        place = jnp.where(low, rest // HALF, beyond // extra)
        quarter = lax.rem(part, 2) * 2 + place // 2
        slab = part // 2 * 2 + lax.rem(place, 2)
        within = jnp.where(low, lax.rem(rest, HALF), HALF + lax.rem(beyond, extra))
        side = jnp.where(stays == 1, other, 1 - other)
        group = group_of(axis, quarter // 2, side, lax.rem(quarter, 2))
        output_row = (group * slabs + slab) * mine + within
        block = output_row // per_slice
        target = jnp.zeros(shape, jnp.int32)
        for s in range(slices):
            target = jnp.where(block == s, owner_ref[s], target)
        breadth = jnp.ones(shape, jnp.int32)
        for s in range(slices):
            breadth = jnp.where(target == s, widths_ref[s], breadth)
        root = 1.0 / jnp.sqrt(breadth.astype(jnp.float32))
        scale[axis] = jnp.broadcast_to(root[peers * mine:], (peers * mine, LANES))
        wanted = target * per_slice + lax.rem(output_row, per_slice)
        for target, cores, extent in ((chosen, 2, live), (chip_chosen, 1, chip_live)):
            wide = lax.broadcasted_iota(jnp.int32, (1, 2 * cores * extent), 1)
            place = lax.rem(wide, extent)
            source = wide // extent
            begin = group_of(axis, source // cores, other, lax.rem(source, cores)) * local_bands
            lowest = jnp.zeros(wide.shape, jnp.int32)
            for s in range(slices):
                lowest = lowest + jnp.where(begin >= ends[s], 1, 0)
            offered = lowest * per_slice + place
            target[axis] = jnp.where(wanted == offered, 1.0, 0.0).astype(jnp.bfloat16)

    known = 0

    def learn():
        pl.semaphore_wait(near.at[known], sides)
        if known + 1 < row_tiles:
            greet_sides(near.at[known + 1])

    for step in range(LEAD, count + UNPACK_LAG):
        if step < count:
            fold(chunks[step])
        if step + 1 < count:
            ready(chunks[step + 1])
            pair_partial(chunks[step + 1])
        if known < row_tiles:
            learn()
            known += 1
        if 0 <= step - MERGE_LAG < count:
            merge(chunks[step - MERGE_LAG])
        if 0 <= step - FAR_LAG < count:
            finish(chunks[step - FAR_LAG], 1)
        if 0 <= step - NEAR_LAG < count:
            cross(chunks[step - NEAR_LAG], 0).start()
        if 0 <= step - FINISH_LAG < count:
            finish(chunks[step - FINISH_LAG], 0)
        if 0 <= step - UNPACK_LAG < count:
            unpack(chunks[step - UNPACK_LAG])

    for names, refs in zip(CHUNK_REFS, groups):
        named = dict(zip(names, refs))
        if "give" in named:
            wait_bytes(named["give"], send1)
            wait_bytes(named["sent"], send1)
        else:
            wait_bytes(named["sent"].at[:, pl.ds(0, 3)], send1)
        wait_bytes(named["came"], send2)
        wait_bytes(named["done"].at[:, pl.ds(0, peers - 1)], send3)


def on_device(groups, slabs, band_coeffs, sign_table, slice_widths, owner_map):
    local_bands, local_columns = band_coeffs.shape
    per_slice = sign_table.shape[0]
    rows = owner_map.shape[0] * per_slice
    tiles, odd = divmod(local_columns, 4 * LANES)
    mine = rows // (8 * slabs)
    reach = (local_bands - 2) // NARROWEST + 2
    chip_reach = (2 * local_bands - 2) // NARROWEST + 2
    live, chip_live = reach * per_slice, chip_reach * per_slice
    fits = 2 * (mine - HALF) == HALF and slabs == HALF and per_slice % HALF == 0
    if groups != 8 or odd or rows % (8 * slabs) or not fits or tiles % 2 or tiles <= NARROW + 2 * LEAD:
        return dense(band_coeffs, sign_table, slice_widths, owner_map)
    peers = 4 * slabs
    extra = mine - HALF

    def buffers(count, tiles, paired):
        width = tiles * LANES
        block = (mine * tiles // HALF, HALF, LANES) if tiles == 2 else (mine // extra, extra, LANES)
        core, chip = [(rows // HALF, HALF, width) for rows in (live, chip_live)]
        shapes = [
            (4, local_bands, width),
            (2, peers * mine, width),
            (peers * mine, width),
            (peers, *block),
            (slabs, 4, *block),
        ]
        shapes += [chip, *[(2, *chip)] * 4] if paired else [(4, *core)] * 2
        return [pltpu.VMEM((count, *shape), jnp.float32) for shape in shapes]

    def aligned(rows):
        return -(-rows // SUBLANES) * SUBLANES

    wide = (tiles - NARROW) // 2 - LEAD
    count = LEAD + wide + NARROW
    return pl.pallas_call(
        functools.partial(kernel, slabs, reach, chip_reach),
        out_shape=pltpu.VMEM((mine, local_columns * slabs), jnp.float32),
        in_specs=[pl.BlockSpec(memory_space=pl.ANY)] * 4,
        out_specs=pl.BlockSpec(memory_space=pltpu.VMEM),
        scratch_shapes=[
            pltpu.SMEM(slice_widths.shape, jnp.int32),
            pltpu.SMEM(owner_map.shape, jnp.int32),
            pltpu.VMEM(sign_table.shape, jnp.int32),
            pltpu.VMEM((aligned(live), local_bands), jnp.bfloat16),
            pltpu.VMEM((aligned(chip_live), local_bands), jnp.bfloat16),
            pltpu.VMEM((2, 2 * peers * mine, 4 * live), jnp.bfloat16),
            pltpu.VMEM((2, 2 * peers * mine, 2 * chip_live), jnp.bfloat16),
            pltpu.VMEM((2, peers * mine, LANES), jnp.float32),
            *buffers(LEAD, 2, False),
            *buffers(wide, 2, True),
            *buffers(NARROW, 1, True),
            pltpu.SemaphoreType.DMA((3,)),
            pltpu.SemaphoreType.DMA((3,)),
            pltpu.SemaphoreType.DMA,
            pltpu.SemaphoreType.DMA((count,)),
            pltpu.SemaphoreType.DMA,
            pltpu.SemaphoreType.DMA((2 * count,)),
            pltpu.SemaphoreType.DMA,
            pltpu.SemaphoreType.DMA((count,)),
            pltpu.SemaphoreType.DMA((count - LEAD,)),
            pltpu.SemaphoreType.REGULAR((slabs - 1,)),
        ],
        compiler_params=pltpu.CompilerParams(
            collective_id=0,
            has_side_effects=True,
            vmem_limit_bytes=VMEM - SUBLANES * local_columns * slabs * 4,
        ),
        name="pseudobands",
    )(slice_widths, owner_map, sign_table, band_coeffs)


def solution(mesh):
    return jax.shard_map(
        functools.partial(on_device, mesh.shape["band"], mesh.shape["gslab"]),
        mesh=mesh,
        in_specs=(P("band", "gslab"), P(None, "band"), P(), P()),
        out_specs=P(("band", "gslab"), None),
        check_vma=False,
    )
```
